256 devices in a mesh: tok: 64 (over x, z, core), tp: 4 (over y).
Axes of the slice: x: 4, y: 4, z: 8, core: 2. Of those that a mesh axis runs over, the one named last changes fastest.
Arguments:
- resid: bfloat16 [8192, 8192], P('tok', 'tp'), may hold values from -7 to 7
- norm_gain: float32 [8192], P('tp'), may hold values from 0.5 to 1.5
- head_in: bfloat16 [8192, 2048], P('tp'), may hold values from -0.088388348 to 0.088388348
- head_bias: float32 [2048], replicated, may hold values from -3 to 3
- head_out: float32 [16, 128], replicated, may hold values from -0.26516504 to 0.26516504
- targets: float32 [8192, 16], P('tok'), may hold values from -12 to 12
- label_mask: int32 [8192, 16], P('tok'), may hold values 0 or 1
- obj_weight: int32 [16], replicated, may hold values from 1 to 16
Outputs:
- resid_grad: bfloat16 [8192, 8192], P('tok', 'tp')
- gain_grad: float32 [8192], P('tp')
- head_in_grad: float32 [8192, 2048], P('tp', 'tok')
- head_bias_grad: float32 [2048], replicated
The draws below stay inside these ranges and needn't reach their ends.
All inputs are finite; a program needn't handle non-finite values. No bound on the sum of `label_mask` on one device may be relied on, other than what follows from the above.
Results may differ from the reference program's by a relative error of at most 0.0078.
Values may be sent and summed in bfloat16 or wider, within the bound.
A program may use at most 128 MiB of HBM per device.

```python
import jax
import jax.numpy as jnp
from jax import lax

D = 8192
OBJ = 16
HH = 128
TOKENS = 8192


def shared_direction(key):
    position = jnp.arange(D, dtype=jnp.float32) / (D - 1)
    feature_ramp = 1.0 + 2.0 * position
    sign_flip = jnp.where(jax.random.bernoulli(jax.random.fold_in(key, 101), 0.5, (D,)), 1.0, -1.0)
    leaning = feature_ramp * sign_flip
    return leaning / jnp.sqrt(jnp.sum(leaning * leaning))


def shared_heads(key):
    return jnp.clip(jax.random.normal(jax.random.fold_in(key, 103), (OBJ, HH), jnp.float32), -3.0, 3.0)


def draw_resid(key, part):
    direction = shared_direction(key)
    strength = jax.random.uniform(jax.random.fold_in(key, 105), (TOKENS, 1), jnp.float32, 0.35, 0.55)
    noise_part = jnp.clip(jax.random.normal(jax.random.fold_in(key, 107), (TOKENS, D), jnp.float32), -5.5, 5.5)
    return jnp.clip(noise_part + strength * D ** 0.5 * direction[None, :], -7.0, 7.0).astype(jnp.bfloat16)


def draw_head_in(key, part):
    direction = shared_direction(key)
    head_base = shared_heads(key)
    scale_in = D ** (-0.5)
    noise_part = jnp.clip(jax.random.normal(jax.random.fold_in(key, 109), (D, OBJ * HH), jnp.float32), -6.0, 6.0)
    leaning = 3.2 * scale_in * direction[:, None] * head_base.reshape(1, OBJ * HH)
    return jnp.clip(noise_part * scale_in + leaning, -8.0 * scale_in, 8.0 * scale_in).astype(jnp.bfloat16)


def draw_head_out(key, part):
    return shared_heads(key) * HH ** (-0.5)


def draw_targets(key, part):
    token_ramp = 1.0 + 2.0 * jnp.arange(TOKENS, dtype=jnp.float32)[:, None] / (TOKENS - 1)
    normal_part = jnp.clip(jax.random.normal(jax.random.fold_in(key, 3), (TOKENS, OBJ), jnp.float32), -4.0, 4.0)
    return normal_part * token_ramp


def with_ends(entries, rng, smallest, high):
    shape = entries.shape
    spot = [jax.random.randint(jax.random.fold_in(rng, axis), (), 0, shape[axis]) for axis in range(len(shape))]
    entries = entries.at[tuple(spot)].set(smallest)
    longest = shape.index(max(shape))
    spot[longest] = (spot[longest] + 1) % shape[longest]
    return entries.at[tuple(spot)].set(high)


def centred(stream_key, shape, scale, reach, kind=jnp.bfloat16):
    return jnp.clip(scale * jax.random.normal(stream_key, shape, jnp.float32), -reach, reach).astype(kind)


def setup_inputs(seed: int = 0) -> dict:
    key_list = jax.random.split(jax.random.key(seed), 9)
    return {
        "resid": draw_resid(jax.random.fold_in(key_list[8], 71), 0),
        "norm_gain": jnp.clip(1.0 + 0.1 * jax.random.normal(key_list[1], (D,), jnp.float32), 0.5, 1.5),
        "head_in": draw_head_in(jax.random.fold_in(key_list[8], 71), 0),
        "head_bias": centred(key_list[3], (OBJ * HH,), 0.5, 3.0, jnp.float32),
        "head_out": draw_head_out(jax.random.fold_in(key_list[8], 71), 0),
        "targets": draw_targets(jax.random.fold_in(key_list[8], 71), 0),
        "label_mask": with_ends((jax.random.randint(key_list[6], (TOKENS, OBJ), 0, 2) < 1).astype(jnp.int32), jax.random.fold_in(key_list[6], 1), 0, 1),
        "obj_weight": with_ends(jax.random.randint(key_list[7], (OBJ,), 1, 17), jax.random.fold_in(key_list[7], 1), 1, 16).astype(jnp.int32),
    }


norm_eps = 1e-05
grad_eps = 1e-06
denominator = 8.0

def reference(resid, norm_gain, head_in, head_bias, head_out, targets, label_mask, obj_weight):
    floated = resid.astype(jnp.float32)
    inverse = lax.rsqrt(lax.optimization_barrier(jnp.sum(floated * floated, axis=1, keepdims=True)) / D + norm_eps)
    unit = floated * inverse
    normed = (unit * norm_gain[None, :]).astype(jnp.bfloat16)
    preact = jnp.dot(normed, head_in, preferred_element_type=jnp.float32) + head_bias[None, :]
    count = preact.shape[0]
    cube = preact.reshape(count, OBJ, HH)
    squash = jax.nn.sigmoid(cube)
    scores = lax.optimization_barrier(jnp.sum(cube * squash * head_out[None], axis=2))
    errors = label_mask.astype(jnp.float32) * (scores - targets)
    slopes = squash * (1.0 + cube * (1.0 - squash))
    row_grad = (errors[:, :, None] * head_out[None] * slopes).astype(jnp.bfloat16)
    grad_cube = row_grad.astype(jnp.float32)
    weight_cube = head_in.astype(jnp.float32).reshape(D, OBJ, HH)
    gram = jnp.einsum('doh,dog->ohg', weight_cube, weight_cube, precision=lax.Precision.HIGHEST)
    mapped = jnp.einsum('toh,ohg->tog', grad_cube, gram, precision=lax.Precision.HIGHEST)
    squares = lax.optimization_barrier(jnp.sum(mapped * grad_cube, axis=(0, 2)))
    obj_rms = jnp.sqrt(squares / (TOKENS * D) + grad_eps)
    balance = obj_weight.astype(jnp.float32) / denominator / obj_rms
    balance_cols = jnp.repeat(balance, HH)
    flat_grad = row_grad.reshape(count, OBJ * HH)
    pre_grad = (flat_grad.astype(jnp.float32) * balance_cols[None, :]).astype(jnp.bfloat16)
    norm_grad = jnp.dot(pre_grad, head_in.T, preferred_element_type=jnp.float32)
    weight_sum = jnp.dot(normed.T, flat_grad, preferred_element_type=jnp.float32)
    head_in_grad = weight_sum * balance_cols[None, :] / TOKENS
    head_bias_grad = lax.optimization_barrier(jnp.sum(flat_grad.astype(jnp.float32), axis=0)) * balance_cols / TOKENS
    gain_grad = lax.optimization_barrier(jnp.sum(norm_grad * unit, axis=0)) / TOKENS
    projection = lax.optimization_barrier(jnp.sum(unit * norm_gain[None, :] * norm_grad, axis=1, keepdims=True)) / D
    resid_grad = (inverse * (norm_gain[None, :] * norm_grad - unit * projection)).astype(jnp.bfloat16)
    return (resid_grad, gain_grad, head_in_grad, head_bias_grad)
```

```python
import functools

import jax
import jax.numpy as jnp
from jax import lax
from jax.experimental import pallas as pl
from jax.experimental.pallas import tpu as pltpu
from jax.sharding import Mesh
from jax.sharding import PartitionSpec as P

TOK = ("tok_0", "tok_1", "tok_2")
F32 = jnp.float32
BF16 = jnp.bfloat16

norm_eps = 1e-05
grad_eps = 1e-06
denominator = 8.0

CHUNKS = 4


def remote(src, dst, send, recv, where):
    return pltpu.make_async_remote_copy(
        src_ref=src,
        dst_ref=dst,
        send_sem=send,
        recv_sem=recv,
        device_id=where,
        device_id_type=pl.DeviceIdType.MESH,
    )


def kernel(
    sizes,
    resid_hbm, head_hbm, gain_ref, bias_ref, hout_ref, tgt_ref, mask_ref, ow_ref,
    dx_hbm, gg_ref, wg_ref, bg_ref,
    resids, head, xb, part, parts_in, sums, sums_in, rg, aux, grad_t, grads, vals, sqp, msg,
    msg_y, msg_x, msg_z, gpart, gmsg, gmsg_x, gmsg_z, wt, stage, inbox, dx_buf,
    load_sem, dx_sem, y_send, y_recv, s_send, s_recv, ag_send, ag_recv, a_send, a_recv,
    r_send, r_recv, t_send, t_recv, qy_send, qy_recv, qx_send, qx_recv, qz_send, qz_recv,
    gx_send, gx_recv, gz_send, gz_recv, w_send, w_recv,
):
    X, Z, C, Y = sizes
    G = X * C
    T, DL = xb.shape
    S = T // Y
    N = head.shape[1]
    O, H = hout_ref.shape
    CW = N // CHUNKS
    D = DL * Y
    tokens = T * X * Z * C
    x, z, c, j = (lax.axis_index(a) for a in (*TOK, "tp"))
    g = x * C + c
    half = Z // 2
    hd = DL // 2

    def at_y(d):
        return {"tp": lax.rem(j + d, Y)}

    def at_xc(e):
        return {"tok_0": lax.rem(x + e // C, X), "tok_2": lax.rem(c + e % C, C)}

    def at_z(d):
        return {"tok_1": lax.rem(z + d, Z)}

    barrier = pltpu.get_barrier_semaphore()
    partners = (
        [at_y(d) for d in range(1, Y)] + [at_xc(e) for e in range(1, G)] + [at_z(d) for d in range(1, Z)]
    )
    for where in partners:
        pl.semaphore_signal(barrier, inc=1, device_id=where, device_id_type=pl.DeviceIdType.MESH)

    def rows_of(group):
        return pl.ds(pl.multiple_of(group * T, T), T)

    mine = rows_of(g)
    load = pltpu.make_async_copy(resid_hbm, resids.at[mine, :], load_sem.at[CHUNKS])
    load.start()
    for n in range(CHUNKS):
        cols = pl.ds(n * CW, CW)
        pltpu.make_async_copy(head_hbm.at[:, cols], head.at[:, cols], load_sem.at[n]).start()
    load.wait()

    total = jnp.zeros((T, 128), F32)
    for i in range(DL // 128):
        lanes = slice(i * 128, (i + 1) * 128)
        r = resids[mine, lanes].astype(F32)
        total = total + r * r
        xb[:, lanes] = (r * gain_ref[:, lanes]).astype(BF16)
    sums[...] = total

    pl.semaphore_wait(barrier, len(partners))

    east, west, twin = {"tok_0": lax.rem(x + 1, X)}, {"tok_0": lax.rem(x + X - 1, X)}, {"tok_2": 1 - c}

    def resid_copy(group, first, count, where, k):
        block = resids.at[pl.ds(pl.multiple_of(group * T + first, count), count), :]
        return remote(block, block, r_send.at[k], r_recv.at[k], where)

    g_west = lax.rem(x + X - 1, X) * C + c
    g_east = lax.rem(x + 1, X) * C + c
    g_far = lax.rem(x + 2, X) * C + c
    far = T // 2
    r_copies = [
        resid_copy(g, 0, T, east, 0),
        resid_copy(g, 0, T, west, 1),
        resid_copy(g, 0, T, twin, 2),
        resid_copy(g_west, 0, far, east, 3),
        resid_copy(g_east, far, far, west, 4),
        resid_copy(g_west, 0, T, twin, 5),
        resid_copy(g_east, 0, T, twin, 6),
        resid_copy(g_far, 0, T, twin, 7),
    ]

    def quarter(k):
        return pl.ds(pl.multiple_of(k * S, S), S)

    own = quarter(j)
    s_copies = []
    for d in range(1, Y):
        to = lax.rem(j + d, Y)
        copy = remote(
            sums.at[quarter(to), :], sums_in.at[d - 1], s_send.at[d - 1], s_recv.at[d - 1], at_y(d)
        )
        copy.start()
        s_copies.append(copy)
    y_copies = []
    for n in range(CHUNKS):
        cols = pl.ds(n * CW, CW)
        pltpu.make_async_copy(head_hbm.at[:, cols], head.at[:, cols], load_sem.at[n]).wait()
        part[:, n * CW : (n + 1) * CW] = jnp.dot(
            xb[...], head[:, n * CW : (n + 1) * CW], preferred_element_type=F32
        ).astype(BF16)
        row = []
        for d in range(1, Y):
            to = lax.rem(j + d, Y)
            copy = remote(
                part.at[quarter(to), cols],
                parts_in.at[d - 1, :, cols],
                y_send.at[d - 1, n],
                y_recv.at[d - 1, n],
                at_y(d),
            )
            copy.start()
            row.append(copy)
        y_copies.append(row)
        if n == 0:
            for k in range(3):
                r_copies[k].start()

    for copy in s_copies:
        copy.wait()
    square = sums[own, :]
    for d in range(Y - 1):
        square = square + sums_in[d]
    inv = lax.rsqrt(jnp.sum(square, axis=1, keepdims=True) / D + norm_eps)

    lane = lax.broadcasted_iota(jnp.int32, (S, 128), 1)
    tgt = tgt_ref[own, :]
    mask = mask_ref[own, :].astype(F32)
    extra = jnp.where(lane == O, inv, 0.0)
    per = O // CHUNKS
    ag_copies = []
    for n in range(CHUNKS):
        cols = pl.ds(n * CW, CW)
        for copy in y_copies[n]:
            copy.wait()
        for o in range(n * per, (n + 1) * per):
            lanes = slice(o * H, (o + 1) * H)
            value = part[own, lanes].astype(F32)
            for d in range(Y - 1):
                value = value + parts_in[d, :, lanes].astype(F32)
            value = value * inv
            cube = value + bias_ref[:, lanes]
            out = hout_ref[o : o + 1, :]
            squash = jax.nn.sigmoid(cube)
            score = jnp.sum(cube * squash * out, axis=1, keepdims=True)
            error = mask[:, o : o + 1] * (score - tgt[:, o : o + 1])
            grad = (error * out * (squash * (1.0 + cube * (1.0 - squash)))).astype(BF16)
            rg[own, lanes] = grad
            moment = jnp.sum(grad.astype(F32) * value, axis=1, keepdims=True)
            extra = jnp.where(lane == o, moment, extra)
        row = []
        for d in range(1, Y):
            block = rg.at[own, cols]
            copy = remote(block, block, ag_send.at[d - 1, n], ag_recv.at[d - 1, n], at_y(d))
            copy.start()
            row.append(copy)
        ag_copies.append(row)
    aux[own, :] = extra
    a_copies = []
    for d in range(1, Y):
        block = aux.at[own, :]
        copy = remote(block, block, a_send.at[d - 1], a_recv.at[d - 1], at_y(d))
        copy.start()
        a_copies.append(copy)

    r_copies[0].wait_recv()
    r_copies[3].start()
    r_copies[5].start()
    r_copies[1].wait_recv()
    r_copies[4].start()
    r_copies[6].start()

    for copy in a_copies:
        copy.wait()
    inverse = aux[:, O : O + 1]
    for n in range(CHUNKS):
        for copy in ag_copies[n]:
            copy.wait()
        for o in range(n * per, (n + 1) * per):
            scaled = rg[:, o * H : (o + 1) * H].astype(F32) * inverse
            flipped = jnp.transpose(scaled).astype(BF16)
            k = o * H // 32
            for b in range(H // 32):
                xx, zz, cc = (k + b) // (Z * C), (k + b) // C % Z, (k + b) % C
                grad_t[xx, zz, cc] = flipped[b * 32 : (b + 1) * 32, :]

    t_copies = []
    for e in range(1, G):
        where = at_xc(e)
        copy = remote(
            grad_t.at[where["tok_0"], :, where["tok_2"]],
            grads.at[g],
            t_send.at[e - 1],
            t_recv.at[e - 1],
            where,
        )
        copy.start()
        t_copies.append(copy)
    grads[g] = grad_t[x, :, c]

    step = 512

    def objective(o, carry):
        lanes = pl.ds(pl.multiple_of(o * H, H), H)
        lhs = rg[:, lanes]
        total = jnp.zeros((8, 128), F32)
        for i in range(DL // step):
            v = lax.dot_general(
                lhs,
                head[i * step : (i + 1) * step, lanes],
                (((1,), (1,)), ((), ())),
                preferred_element_type=F32,
            )
            vals[o, :, i * step : (i + 1) * step] = v
            for k in range(step // 128):
                w = v[:, k * 128 : (k + 1) * 128]
                total = total + jnp.sum((w * w).reshape(T // 8, 8, 128), axis=0)
        sqp[o] = total
        return carry

    lax.fori_loop(0, O, objective, 0)
    msg[0:O, :] = jnp.sum(sqp[...], axis=1)
    for o in range(O):
        msg[O + o : O + o + 1, :] = jnp.sum(
            rg[:, o * H : (o + 1) * H].astype(F32), axis=0, keepdims=True
        )

    msg_y[j] = msg[0:O, :]
    qy = []
    for d in range(1, Y):
        copy = remote(
            msg.at[0:O, :], msg_y.at[j], qy_send.at[d - 1], qy_recv.at[d - 1], at_y(d)
        )
        copy.start()
        qy.append(copy)

    r_copies[3].wait_recv()
    r_copies[4].wait_recv()
    r_copies[7].start()
    for k in (2, 5, 6, 7):
        r_copies[k].wait_recv()
    for copy in t_copies:
        copy.wait()

    wstep = 256

    def weight(i, carry):
        lanes = pl.ds(pl.multiple_of(i * wstep, wstep), wstep)
        lhs = jnp.concatenate([grads[k].reshape(Z * 32, T) for k in range(G)], axis=1)
        v = jnp.dot(lhs, resids[:, lanes], preferred_element_type=F32)
        wt[:, :, lanes] = v.reshape(Z, 32, wstep)
        return carry

    chains = ((0, 1, half), (1, -1, half), (1, 1, half - 1), (0, -1, half - 1))
    base = (0, half, 2 * half, 3 * half - 1)

    def chain_copy(k, s):
        _, direction, _ = chains[k]
        slot = base[k] + s
        return remote(
            stage.at[slot],
            inbox.at[slot],
            w_send.at[slot],
            w_recv.at[slot],
            at_z(1 if direction > 0 else Z - 1),
        )

    def chain_step(k, s):
        part_of, direction, count = chains[k]
        distance = count - s
        owner = lax.rem(z + (distance if direction > 0 else Z - distance), Z)
        lanes = slice(part_of * hd, (part_of + 1) * hd)
        value = wt[owner, :, lanes]
        if s > 0:
            chain_copy(k, s - 1).wait_recv()
            value = value + inbox[base[k] + s - 1].astype(F32)
        stage[base[k] + s] = value.astype(BF16)
        chain_copy(k, s).start()

    lax.fori_loop(0, hd // wstep, weight, 0)
    chain_step(0, 0)
    chain_step(3, 0)
    lax.fori_loop(hd // wstep, DL // wstep, weight, 0)
    chain_step(1, 0)
    chain_step(2, 0)

    def round_of(s):
        for k in range(4):
            if s < chains[k][2]:
                chain_step(k, s)

    for copy in qy:
        copy.wait()
    squares = msg_y[0]
    for k in range(1, Y):
        squares = squares + msg_y[k]
    msg[0:O, :] = squares
    msg_x[g] = msg[...]
    qx = []
    for e in range(1, G):
        copy = remote(msg, msg_x.at[g], qx_send.at[e - 1], qx_recv.at[e - 1], at_xc(e))
        copy.start()
        qx.append(copy)
    if half > 1:
        round_of(1)
    for copy in qx:
        copy.wait()
    both = msg_x[0]
    for k in range(1, G):
        both = both + msg_x[k]
    msg_z[z] = both
    qz = []
    for d in range(1, Z):
        copy = remote(msg_z.at[z], msg_z.at[z], qz_send.at[d - 1], qz_recv.at[d - 1], at_z(d))
        copy.start()
        qz.append(copy)
    if half > 2:
        round_of(2)
    for copy in qz:
        copy.wait()
    both = msg_z[0]
    for k in range(1, Z):
        both = both + msg_z[k]
    eye = lax.broadcasted_iota(jnp.int32, (O, 128), 0) == lax.broadcasted_iota(jnp.int32, (O, 128), 1)
    eye16 = lax.broadcasted_iota(jnp.int32, (O, O), 0) == lax.broadcasted_iota(jnp.int32, (O, O), 1)
    squares = jnp.sum(both[0:O, :], axis=1, keepdims=True)
    weights = jnp.sum(jnp.where(eye16, ow_ref[...].astype(F32), 0.0), axis=1, keepdims=True)
    balance = weights / denominator / jnp.sqrt(squares / (tokens * D) + grad_eps)
    balance_row = jnp.sum(jnp.where(eye, balance, 0.0), axis=0, keepdims=True)
    bg_ref[...] = both[O : 2 * O, :] * balance / tokens

    inverse = aux[:, O : O + 1]
    projection = jnp.sum(
        jnp.where(lax.broadcasted_iota(jnp.int32, (T, 128), 1) < O, aux[...] * balance_row, 0.0),
        axis=1,
        keepdims=True,
    )
    shrink = projection / D
    factors = [jnp.broadcast_to(balance[o : o + 1, :], (8, 128)) for o in range(O)]

    def combine(i, carry):
        lanes = pl.ds(pl.multiple_of(i * 128, 128), 128)
        norm = jnp.zeros((T // 8, 8, 128), F32)
        for o in range(O):
            norm = norm + vals[o, :, lanes].reshape(T // 8, 8, 128) * factors[o][None]
        norm = norm.reshape(T, 128)
        unit = resids[mine, lanes].astype(F32) * inverse
        gpart[i] = jnp.sum((norm * unit).reshape(T // 8, 8, 128), axis=0)
        dx_buf[:, lanes] = (inverse * (gain_ref[:, lanes] * norm - unit * shrink)).astype(BF16)
        return carry

    lax.fori_loop(0, DL // 128, combine, 0)
    dx_copy = pltpu.make_async_copy(dx_buf, dx_hbm, dx_sem)
    dx_copy.start()
    gmsg[...] = jnp.sum(gpart[...], axis=1)
    gmsg_x[g] = gmsg[...]
    gx = []
    for e in range(1, G):
        copy = remote(gmsg, gmsg_x.at[g], gx_send.at[e - 1], gx_recv.at[e - 1], at_xc(e))
        copy.start()
        gx.append(copy)
    for s in range(3, half):
        round_of(s)
    for copy in gx:
        copy.wait()
    both = gmsg_x[0]
    for k in range(1, G):
        both = both + gmsg_x[k]
    gmsg_z[z] = both
    gz = []
    for d in range(1, Z):
        copy = remote(gmsg_z.at[z], gmsg_z.at[z], gz_send.at[d - 1], gz_recv.at[d - 1], at_z(d))
        copy.start()
        gz.append(copy)

    k_own = (x * Z + z) * C + c
    objective_own = k_own * 32 // H
    scale = jnp.sum(
        jnp.where(lax.broadcasted_iota(jnp.int32, (O, 1), 0) == objective_own, balance, 0.0),
        axis=0,
        keepdims=True,
    )
    for part_of in range(2):
        lanes = slice(part_of * hd, (part_of + 1) * hd)
        value = wt[z, :, lanes]
        for k in range(4):
            if chains[k][0] == part_of and chains[k][2] > 0:
                chain_copy(k, chains[k][2] - 1).wait_recv()
                value = value + inbox[base[k] + chains[k][2] - 1].astype(F32)
        wg_ref[:, lanes] = value * gain_ref[:, lanes] * scale / tokens

    for copy in gz:
        copy.wait()
    both = gmsg_z[0]
    for k in range(1, Z):
        both = both + gmsg_z[k]
    gg_ref[...] = both / tokens

    for copy in r_copies:
        copy.wait_send()
    for k in range(4):
        for s in range(chains[k][2]):
            chain_copy(k, s).wait_send()
    dx_copy.wait()


def per_device(resid, norm_gain, head_in, head_bias, head_out, targets, label_mask, obj_weight):
    X, Z, C, Y = (lax.axis_size(a) for a in (*TOK, "tp"))
    G = X * C
    T, DL = resid.shape
    N = head_in.shape[1]
    O, H = head_out.shape
    S = T // Y
    CW = N // CHUNKS
    columns = N // (X * Z * C)
    slots = 2 * (Z - 1)
    any_space = pl.BlockSpec(memory_space=pl.ANY)
    vmem = pl.BlockSpec(memory_space=pltpu.VMEM)
    dma = pltpu.SemaphoreType.DMA
    V = pltpu.VMEM
    scratch = [
        V((G * T, DL), BF16),
        V((DL, N), BF16),
        V((T, DL), BF16),
        V((T, N), BF16),
        V((Y - 1, S, N), BF16),
        V((T, 128), F32),
        V((Y - 1, S, 128), F32),
        V((T, N), BF16),
        V((T, 128), F32),
        V((X, Z, C, columns, T), BF16),
        V((G, Z, columns, T), BF16),
        V((O, T, DL), F32),
        V((O, 8, 128), F32),
        V((2 * O, 128), F32),
        V((Y, O, 128), F32),
        V((G, 2 * O, 128), F32),
        V((Z, 2 * O, 128), F32),
        V((DL // 128, 8, 128), F32),
        V((DL // 128, 128), F32),
        V((G, DL // 128, 128), F32),
        V((Z, DL // 128, 128), F32),
        V((Z, columns, DL), F32),
        V((slots, columns, DL // 2), BF16),
        V((slots, columns, DL // 2), BF16),
        V((T, DL), BF16),
        dma((CHUNKS + 1,)),
        dma,
        dma((Y - 1, CHUNKS)), dma((Y - 1, CHUNKS)),
        dma((Y - 1,)), dma((Y - 1,)),
        dma((Y - 1, CHUNKS)), dma((Y - 1, CHUNKS)),
        dma((Y - 1,)), dma((Y - 1,)),
        dma((8,)), dma((8,)),
        dma((G - 1,)), dma((G - 1,)),
        dma((Y - 1,)), dma((Y - 1,)),
        dma((G - 1,)), dma((G - 1,)),
        dma((Z - 1,)), dma((Z - 1,)),
        dma((G - 1,)), dma((G - 1,)),
        dma((Z - 1,)), dma((Z - 1,)),
        dma((slots,)), dma((slots,)),
    ]
    dx, gg, wg, bg = pl.pallas_call(
        functools.partial(kernel, (X, Z, C, Y)),
        out_shape=(
            jax.ShapeDtypeStruct((T, DL), BF16),
            jax.ShapeDtypeStruct((DL // 128, 128), F32),
            jax.ShapeDtypeStruct((columns, DL), F32),
            jax.ShapeDtypeStruct((O, H), F32),
        ),
        in_specs=[any_space, any_space] + [vmem] * 6,
        out_specs=(any_space, vmem, vmem, vmem),
        scratch_shapes=scratch,
        compiler_params=pltpu.CompilerParams(
            collective_id=0, has_side_effects=True, vmem_limit_bytes=60 << 20
        ),
    )(
        resid,
        head_in,
        norm_gain.reshape(1, DL),
        head_bias.reshape(1, N),
        head_out,
        targets,
        label_mask,
        obj_weight.reshape(1, O),
    )
    return dx, gg.reshape(DL), wg.T, bg.reshape(N)


def solution(mesh):
    finer = Mesh(mesh.devices.reshape(4, 8, 2, mesh.shape["tp"]), ("tok_0", "tok_1", "tok_2", "tp"))
    placed = (P(TOK, "tp"), P("tp"), P("tp", None), P(), P(), P(TOK, None), P(TOK, None), P())
    return jax.shard_map(
        per_device,
        mesh=finer,
        in_specs=placed,
        out_specs=(P(TOK, "tp"), P("tp"), P("tp", TOK), P()),
        check_vma=False,
    )
```

```python
import functools

import jax
import jax.numpy as jnp
from jax import lax
from jax.experimental import pallas as pl
from jax.experimental.pallas import tpu as pltpu
from jax.sharding import Mesh
from jax.sharding import PartitionSpec as P

TOK = ("tok_0", "tok_1", "tok_2")
F32 = jnp.float32
BF16 = jnp.bfloat16

norm_eps = 1e-05
grad_eps = 1e-06
denominator = 8.0

CHUNKS = 4


def remote(src, dst, send, recv, where):
    return pltpu.make_async_remote_copy(
        src_ref=src,
        dst_ref=dst,
        send_sem=send,
        recv_sem=recv,
        device_id=where,
        device_id_type=pl.DeviceIdType.MESH,
    )


def kernel(
    sizes,
    resid_hbm, head_hbm, gain_hbm, bias_hbm, hout_hbm, tgt_hbm, mask_hbm, ow_hbm,
    dx_ref, gg_ref, wg_ref, bg_ref,
    gain_ref, bias_ref, hout_ref, tgt_ref, mask_ref, ow_ref,
    tgt_t, mask_t, resids, head, xb, part, parts_in, sums, sums_in, rg, aux, grad_t, grads, vals, sqp, msg,
    msg_y, msg_x, msg_z, gpart, gmsg, gmsg_x, gmsg_z, wt, stage, inbox,
    load_sem, small_sem, y_send, y_recv, s_send, s_recv, ag_send, ag_recv, a_send, a_recv,
    r_send, r_recv, t_send, t_recv, qy_send, qy_recv, qx_send, qx_recv, qz_send, qz_recv,
    gx_send, gx_recv, gz_send, gz_recv, w_send, w_recv,
):
    X, Z, C, Y = sizes
    G = X * C
    T, DL = xb.shape
    S = T // Y
    N = head.shape[1]
    O, H = hout_ref.shape
    CW = N // CHUNKS
    D = DL * Y
    tokens = T * X * Z * C
    x, z, c, j = (lax.axis_index(a) for a in (*TOK, "tp"))
    g = x * C + c
    half = Z // 2
    hd = DL // 2

    def at_y(d):
        return {"tp": lax.rem(j + d, Y)}

    def at_xc(e):
        return {"tok_0": lax.rem(x + e // C, X), "tok_2": lax.rem(c + e % C, C)}

    def at_z(d):
        return {"tok_1": lax.rem(z + d, Z)}

    barrier = pltpu.get_barrier_semaphore()
    partners = (
        [at_y(d) for d in range(1, Y)] + [at_xc(e) for e in range(1, G)] + [at_z(d) for d in range(1, Z)]
    )
    for where in partners:
        pl.semaphore_signal(barrier, inc=1, device_id=where, device_id_type=pl.DeviceIdType.MESH)

    def rows_of(group):
        return pl.ds(pl.multiple_of(group * T, T), T)

    mine = rows_of(g)
    load = pltpu.make_async_copy(resid_hbm, resids.at[mine, :], load_sem.at[CHUNKS])
    load.start()
    small = [
        pltpu.make_async_copy(src, dst, small_sem.at[k])
        for k, (src, dst) in enumerate(
            (
                (gain_hbm, gain_ref),
                (bias_hbm, bias_ref),
                (hout_hbm, hout_ref),
                (tgt_hbm, tgt_ref),
                (mask_hbm, mask_ref),
                (ow_hbm, ow_ref),
            )
        )
    ]
    for copy in small:
        copy.start()
    for n in range(CHUNKS):
        cols = pl.ds(n * CW, CW)
        pltpu.make_async_copy(head_hbm.at[:, cols], head.at[:, cols], load_sem.at[n]).start()
    for copy in small:
        copy.wait()
    tgt_t[...] = jnp.transpose(tgt_ref[...])
    mask_t[...] = jnp.transpose(mask_ref[...].astype(F32))
    load.wait()

    total = jnp.zeros((T, 128), F32)
    for i in range(DL // 128):
        lanes = slice(i * 128, (i + 1) * 128)
        r = resids[mine, lanes].astype(F32)
        total = total + r * r
        xb[:, lanes] = (r * gain_ref[:, lanes]).astype(BF16)
    sums[...] = total

    pl.semaphore_wait(barrier, len(partners))

    east, west, twin = {"tok_0": lax.rem(x + 1, X)}, {"tok_0": lax.rem(x + X - 1, X)}, {"tok_2": 1 - c}

    def resid_copy(group, first, count, where, k):
        block = resids.at[pl.ds(pl.multiple_of(group * T + first, count), count), :]
        return remote(block, block, r_send.at[k], r_recv.at[k], where)

    g_west = lax.rem(x + X - 1, X) * C + c
    g_east = lax.rem(x + 1, X) * C + c
    g_far = lax.rem(x + 2, X) * C + c
    far = T // 2
    r_copies = [
        resid_copy(g, 0, far, east, 0),
        resid_copy(g, far, far, west, 1),
        resid_copy(g, far, far, east, 2),
        resid_copy(g, 0, far, west, 3),
        resid_copy(g, 0, T, twin, 4),
        resid_copy(g_west, 0, far, east, 5),
        resid_copy(g_east, far, far, west, 6),
        resid_copy(g_west, 0, T, twin, 7),
        resid_copy(g_east, 0, T, twin, 8),
        resid_copy(g_far, 0, T, twin, 9),
    ]

    def quarter(k):
        return pl.ds(pl.multiple_of(k * S, S), S)

    own = quarter(j)
    s_copies = []
    for d in range(1, Y):
        to = lax.rem(j + d, Y)
        copy = remote(
            sums.at[quarter(to), :], sums_in.at[d - 1], s_send.at[d - 1], s_recv.at[d - 1], at_y(d)
        )
        copy.start()
        s_copies.append(copy)
    y_copies = []
    for n in range(CHUNKS):
        cols = pl.ds(n * CW, CW)
        pltpu.make_async_copy(head_hbm.at[:, cols], head.at[:, cols], load_sem.at[n]).wait()
        part[:, n * CW : (n + 1) * CW] = jnp.dot(
            xb[...], head[:, n * CW : (n + 1) * CW], preferred_element_type=F32
        ).astype(BF16)
        row = []
        for d in range(1, Y):
            to = lax.rem(j + d, Y)
            copy = remote(
                part.at[quarter(to), cols],
                parts_in.at[d - 1, :, cols],
                y_send.at[d - 1, n],
                y_recv.at[d - 1, n],
                at_y(d),
            )
            copy.start()
            row.append(copy)
        y_copies.append(row)
        if n == 0:
            for k in range(5):
                r_copies[k].start()

    for copy in s_copies:
        copy.wait()
    square = sums[own, :]
    for d in range(Y - 1):
        square = square + sums_in[d]
    inv = lax.rsqrt(jnp.sum(square, axis=1, keepdims=True) / D + norm_eps)

    lane = lax.broadcasted_iota(jnp.int32, (S, 128), 1)
    tgt = tgt_t[own, :]
    mask = mask_t[own, :]
    extra = jnp.where(lane == O, inv, 0.0)
    per = O // CHUNKS
    ag_copies = []
    for n in range(CHUNKS):
        cols = pl.ds(n * CW, CW)
        for copy in y_copies[n]:
            copy.wait()
        for o in range(n * per, (n + 1) * per):
            lanes = slice(o * H, (o + 1) * H)
            value = part[own, lanes].astype(F32)
            for d in range(Y - 1):
                value = value + parts_in[d, :, lanes].astype(F32)
            value = value * inv
            cube = value + bias_ref[:, lanes]
            out = hout_ref[o : o + 1, :]
            squash = jax.nn.sigmoid(cube)
            score = jnp.sum(cube * squash * out, axis=1, keepdims=True)
            error = mask[:, o : o + 1] * (score - tgt[:, o : o + 1])
            grad = (error * out * (squash * (1.0 + cube * (1.0 - squash)))).astype(BF16)
            rg[own, lanes] = grad
            moment = jnp.sum(grad.astype(F32) * value, axis=1, keepdims=True)
            extra = jnp.where(lane == o, moment, extra)
        row = []
        for d in range(1, Y):
            block = rg.at[own, cols]
            copy = remote(block, block, ag_send.at[d - 1, n], ag_recv.at[d - 1, n], at_y(d))
            copy.start()
            row.append(copy)
        ag_copies.append(row)
    aux[own, :] = extra
    a_copies = []
    for d in range(1, Y):
        block = aux.at[own, :]
        copy = remote(block, block, a_send.at[d - 1], a_recv.at[d - 1], at_y(d))
        copy.start()
        a_copies.append(copy)

    r_copies[0].wait_recv()
    r_copies[5].start()
    r_copies[1].wait_recv()
    r_copies[6].start()

    for copy in a_copies:
        copy.wait()
    inverse = aux[:, O : O + 1]
    for n in range(CHUNKS):
        for copy in ag_copies[n]:
            copy.wait()
        for o in range(n * per, (n + 1) * per):
            scaled = rg[:, o * H : (o + 1) * H].astype(F32) * inverse
            flipped = jnp.transpose(scaled).astype(BF16)
            k = o * H // 32
            for b in range(H // 32):
                xx, zz, cc = (k + b) // (Z * C), (k + b) // C % Z, (k + b) % C
                grad_t[xx, zz, cc] = flipped[b * 32 : (b + 1) * 32, :]

    t_copies = []
    for e in range(1, G):
        where = at_xc(e)
        copy = remote(
            grad_t.at[where["tok_0"], :, where["tok_2"]],
            grads.at[g],
            t_send.at[e - 1],
            t_recv.at[e - 1],
            where,
        )
        copy.start()
        t_copies.append(copy)
    grads[g] = grad_t[x, :, c]

    r_copies[2].wait_recv()
    r_copies[7].start()
    r_copies[3].wait_recv()
    r_copies[8].start()

    step = 512

    def objective(o, carry):
        lanes = pl.ds(pl.multiple_of(o * H, H), H)
        lhs = rg[:, lanes]
        total = jnp.zeros((8, 128), F32)
        for i in range(DL // step):
            v = lax.dot_general(
                lhs,
                head[i * step : (i + 1) * step, lanes],
                (((1,), (1,)), ((), ())),
                preferred_element_type=F32,
            )
            vals[o, :, i * step : (i + 1) * step] = v
            for k in range(step // 128):
                w = v[:, k * 128 : (k + 1) * 128]
                total = total + jnp.sum((w * w).reshape(T // 8, 8, 128), axis=0)
        sqp[o] = total
        return carry

    lax.fori_loop(0, O, objective, 0)
    msg[0:O, :] = jnp.sum(sqp[...], axis=1)
    for o in range(O):
        msg[O + o : O + o + 1, :] = jnp.sum(
            rg[:, o * H : (o + 1) * H].astype(F32), axis=0, keepdims=True
        )

    msg_y[j] = msg[0:O, :]
    qy = []
    for d in range(1, Y):
        copy = remote(
            msg.at[0:O, :], msg_y.at[j], qy_send.at[d - 1], qy_recv.at[d - 1], at_y(d)
        )
        copy.start()
        qy.append(copy)

    r_copies[5].wait_recv()
    r_copies[6].wait_recv()
    r_copies[9].start()
    for copy in qy:
        copy.wait()
    squares = msg_y[0]
    for k in range(1, Y):
        squares = squares + msg_y[k]
    msg[0:O, :] = squares
    msg_x[g] = msg[...]
    qx = []
    for e in range(1, G):
        copy = remote(msg, msg_x.at[g], qx_send.at[e - 1], qx_recv.at[e - 1], at_xc(e))
        copy.start()
        qx.append(copy)
    for k in (4, 7, 8, 9):
        r_copies[k].wait_recv()
    for copy in t_copies:
        copy.wait()

    wstep = 256

    def weight(i, carry):
        lanes = pl.ds(pl.multiple_of(i * wstep, wstep), wstep)
        lhs = jnp.concatenate([grads[k].reshape(Z * 32, T) for k in range(G)], axis=1)
        v = jnp.dot(lhs, resids[:, lanes], preferred_element_type=F32)
        wt[:, :, lanes] = v.reshape(Z, 32, wstep)
        return carry

    chains = ((0, 1, half), (1, -1, half), (1, 1, half - 1), (0, -1, half - 1))
    base = (0, half, 2 * half, 3 * half - 1)

    def chain_copy(k, s):
        _, direction, _ = chains[k]
        slot = base[k] + s
        return remote(
            stage.at[slot],
            inbox.at[slot],
            w_send.at[slot],
            w_recv.at[slot],
            at_z(1 if direction > 0 else Z - 1),
        )

    def chain_step(k, s):
        part_of, direction, count = chains[k]
        distance = count - s
        owner = lax.rem(z + (distance if direction > 0 else Z - distance), Z)
        lanes = slice(part_of * hd, (part_of + 1) * hd)
        value = wt[owner, :, lanes]
        if s > 0:
            chain_copy(k, s - 1).wait_recv()
            value = value + inbox[base[k] + s - 1].astype(F32)
        stage[base[k] + s] = value.astype(BF16)
        chain_copy(k, s).start()

    lax.fori_loop(0, hd // wstep, weight, 0)
    chain_step(0, 0)
    chain_step(3, 0)

    for copy in qx:
        copy.wait()
    both = msg_x[0]
    for k in range(1, G):
        both = both + msg_x[k]
    msg_z[z] = both
    qz = []
    for d in range(1, Z):
        copy = remote(msg_z.at[z], msg_z.at[z], qz_send.at[d - 1], qz_recv.at[d - 1], at_z(d))
        copy.start()
        qz.append(copy)

    lax.fori_loop(hd // wstep, DL // wstep, weight, 0)
    chain_step(1, 0)
    chain_step(2, 0)

    def round_of(s):
        for k in range(4):
            if s < chains[k][2]:
                chain_step(k, s)

    if half > 1:
        round_of(1)
    for copy in qz:
        copy.wait()
    both = msg_z[0]
    for k in range(1, Z):
        both = both + msg_z[k]
    eye = lax.broadcasted_iota(jnp.int32, (O, 128), 0) == lax.broadcasted_iota(jnp.int32, (O, 128), 1)
    eye16 = lax.broadcasted_iota(jnp.int32, (O, O), 0) == lax.broadcasted_iota(jnp.int32, (O, O), 1)
    squares = jnp.sum(both[0:O, :], axis=1, keepdims=True)
    weights = jnp.sum(jnp.where(eye16, ow_ref[...].astype(F32), 0.0), axis=1, keepdims=True)
    balance = weights / denominator / jnp.sqrt(squares / (tokens * D) + grad_eps)
    balance_row = jnp.sum(jnp.where(eye, balance, 0.0), axis=0, keepdims=True)
    bg_ref[...] = both[O : 2 * O, :] * balance / tokens

    inverse = aux[:, O : O + 1]
    projection = jnp.sum(
        jnp.where(lax.broadcasted_iota(jnp.int32, (T, 128), 1) < O, aux[...] * balance_row, 0.0),
        axis=1,
        keepdims=True,
    )
    shrink = projection / D
    factors = [jnp.broadcast_to(balance[o : o + 1, :], (8, 128)) for o in range(O)]

    def combine(i, carry):
        lanes = pl.ds(pl.multiple_of(i * 128, 128), 128)
        norm = jnp.zeros((T // 8, 8, 128), F32)
        for o in range(O):
            norm = norm + vals[o, :, lanes].reshape(T // 8, 8, 128) * factors[o][None]
        norm = norm.reshape(T, 128)
        unit = resids[mine, lanes].astype(F32) * inverse
        gpart[i] = jnp.sum((norm * unit).reshape(T // 8, 8, 128), axis=0)
        dx_ref[:, lanes] = (inverse * (gain_ref[:, lanes] * norm - unit * shrink)).astype(BF16)
        return carry

    lax.fori_loop(0, DL // 128, combine, 0)
    gmsg[...] = jnp.sum(gpart[...], axis=1)
    gmsg_x[g] = gmsg[...]
    gx = []
    for e in range(1, G):
        copy = remote(gmsg, gmsg_x.at[g], gx_send.at[e - 1], gx_recv.at[e - 1], at_xc(e))
        copy.start()
        gx.append(copy)
    if half > 2:
        round_of(2)
    for copy in gx:
        copy.wait()
    both = gmsg_x[0]
    for k in range(1, G):
        both = both + gmsg_x[k]
    gmsg_z[z] = both
    gz = []
    for d in range(1, Z):
        copy = remote(gmsg_z.at[z], gmsg_z.at[z], gz_send.at[d - 1], gz_recv.at[d - 1], at_z(d))
        copy.start()
        gz.append(copy)

    for s in range(3, half):
        round_of(s)

    k_own = (x * Z + z) * C + c
    objective_own = k_own * 32 // H
    scale = jnp.sum(
        jnp.where(lax.broadcasted_iota(jnp.int32, (O, 1), 0) == objective_own, balance, 0.0),
        axis=0,
        keepdims=True,
    )
    for part_of in range(2):
        lanes = slice(part_of * hd, (part_of + 1) * hd)
        value = wt[z, :, lanes]
        for k in range(4):
            if chains[k][0] == part_of and chains[k][2] > 0:
                chain_copy(k, chains[k][2] - 1).wait_recv()
                value = value + inbox[base[k] + chains[k][2] - 1].astype(F32)
        wg_ref[:, lanes] = value * gain_ref[:, lanes] * scale / tokens

    for copy in gz:
        copy.wait()
    both = gmsg_z[0]
    for k in range(1, Z):
        both = both + gmsg_z[k]
    gg_ref[...] = both / tokens

    for copy in r_copies:
        copy.wait_send()
    for k in range(4):
        for s in range(chains[k][2]):
            chain_copy(k, s).wait_send()


def settle(dx_ref, gg_ref, wg_ref, bg_ref, dx_out, gg_out, wg_out, bg_out):
    dx_out[...] = dx_ref[...]
    gg_out[...] = gg_ref[...]
    wg_out[...] = wg_ref[...]
    bg_out[...] = bg_ref[...]


def per_device(resid, norm_gain, head_in, head_bias, head_out, targets, label_mask, obj_weight):
    X, Z, C, Y = (lax.axis_size(a) for a in (*TOK, "tp"))
    G = X * C
    T, DL = resid.shape
    N = head_in.shape[1]
    O, H = head_out.shape
    S = T // Y
    CW = N // CHUNKS
    columns = N // (X * Z * C)
    slots = 2 * (Z - 1)
    hbm = pl.BlockSpec(memory_space=pltpu.HBM)
    vmem = pl.BlockSpec(memory_space=pltpu.VMEM)
    dma = pltpu.SemaphoreType.DMA
    V = pltpu.VMEM
    scratch = [
        V((1, DL), F32),
        V((1, N), F32),
        V((O, H), F32),
        V((O, T), F32),
        V((O, T), jnp.int32),
        V((1, O), jnp.int32),
        V((T, O), F32),
        V((T, O), F32),
        V((G * T, DL), BF16),
        V((DL, N), BF16),
        V((T, DL), BF16),
        V((T, N), BF16),
        V((Y - 1, S, N), BF16),
        V((T, 128), F32),
        V((Y - 1, S, 128), F32),
        V((T, N), BF16),
        V((T, 128), F32),
        V((X, Z, C, columns, T), BF16),
        V((G, Z, columns, T), BF16),
        V((O, T, DL), F32),
        V((O, 8, 128), F32),
        V((2 * O, 128), F32),
        V((Y, O, 128), F32),
        V((G, 2 * O, 128), F32),
        V((Z, 2 * O, 128), F32),
        V((DL // 128, 8, 128), F32),
        V((DL // 128, 128), F32),
        V((G, DL // 128, 128), F32),
        V((Z, DL // 128, 128), F32),
        V((Z, columns, DL), F32),
        V((slots, columns, DL // 2), BF16),
        V((slots, columns, DL // 2), BF16),
        dma((CHUNKS + 1,)), dma((6,)),
        dma((Y - 1, CHUNKS)), dma((Y - 1, CHUNKS)),
        dma((Y - 1,)), dma((Y - 1,)),
        dma((Y - 1, CHUNKS)), dma((Y - 1, CHUNKS)),
        dma((Y - 1,)), dma((Y - 1,)),
        dma((10,)), dma((10,)),
        dma((G - 1,)), dma((G - 1,)),
        dma((Y - 1,)), dma((Y - 1,)),
        dma((G - 1,)), dma((G - 1,)),
        dma((Z - 1,)), dma((Z - 1,)),
        dma((G - 1,)), dma((G - 1,)),
        dma((Z - 1,)), dma((Z - 1,)),
        dma((slots,)), dma((slots,)),
    ]
    dx, gg, wg, bg = pl.pallas_call(
        functools.partial(kernel, (X, Z, C, Y)),
        out_shape=(
            jax.ShapeDtypeStruct((T, DL), BF16),
            jax.ShapeDtypeStruct((DL // 128, 128), F32),
            jax.ShapeDtypeStruct((columns, DL), F32),
            jax.ShapeDtypeStruct((O, H), F32),
        ),
        in_specs=[hbm] * 8,
        out_specs=(vmem,) * 4,
        scratch_shapes=scratch,
        compiler_params=pltpu.CompilerParams(
            collective_id=0, has_side_effects=True, vmem_limit_bytes=48 << 20
        ),
    )(
        *(
            pltpu.with_memory_space_constraint(a, pltpu.HBM)
            for a in (
                resid,
                head_in,
                norm_gain.reshape(1, DL),
                head_bias.reshape(1, N),
                head_out,
                targets.T,
                label_mask.T,
                obj_weight.reshape(1, O),
            )
        )
    )
    dx, gg, wg, bg = pl.pallas_call(
        settle,
        out_shape=tuple(jax.ShapeDtypeStruct(a.shape, a.dtype) for a in (dx, gg, wg, bg)),
        in_specs=[vmem] * 4,
        out_specs=(vmem,) * 4,
        compiler_params=pltpu.CompilerParams(vmem_limit_bytes=4 << 20),
    )(dx, gg, wg, bg)
    return dx, gg.reshape(DL), wg.T, bg.reshape(N)


def solution(mesh):
    finer = Mesh(mesh.devices.reshape(4, 8, 2, mesh.shape["tp"]), ("tok_0", "tok_1", "tok_2", "tp"))
    placed = (P(TOK, "tp"), P("tp"), P("tp", None), P(), P(), P(TOK, None), P(TOK, None), P())
    return jax.shard_map(
        per_device,
        mesh=finer,
        in_specs=placed,
        out_specs=(P(TOK, "tp"), P("tp"), P("tp", TOK), P()),
        check_vma=False,
    )
```

```python
import functools

import jax
import jax.numpy as jnp
from jax import lax
from jax.experimental import pallas as pl
from jax.experimental.pallas import tpu as pltpu
from jax.sharding import Mesh
from jax.sharding import PartitionSpec as P

TOK = ("tok_0", "tok_1", "tok_2")
F32 = jnp.float32
BF16 = jnp.bfloat16

norm_eps = 1e-05
grad_eps = 1e-06
denominator = 8.0

STEPS = (2, 1, 3, 0)
CHUNKS = len(STEPS)


def remote(src, dst, send, recv, where):
    return pltpu.make_async_remote_copy(
        src_ref=src,
        dst_ref=dst,
        send_sem=send,
        recv_sem=recv,
        device_id=where,
        device_id_type=pl.DeviceIdType.MESH,
    )


def kernel(
    sizes,
    resid_hbm, head_hbm, gain_hbm, bias_hbm, hout_hbm, tgt_hbm, mask_hbm, ow_hbm,
    dx_ref, gg_ref, wg_ref, bg_ref,
    gain_ref, bias_ref, hout_ref, tgt_ref, mask_ref, ow_ref,
    tgt_t, mask_t, resids, head, xb, part, parts_in, sums, sums_in, rg, aux, inverses, grad_t, grads, vals, sqp,
    msg_b, msg_y, msg_x, msg_z, gpart, gmsg, gmsg_x, gmsg_z, wt, stage, inbox,
    load_sem, small_sem, y_send, y_recv, s_send, s_recv, ag_send, ag_recv, a_send, a_recv, i_send, i_recv,
    r_send, r_recv, t_send, t_recv, qy_send, qy_recv, qx_send, qx_recv, qz_send, qz_recv, qb_send, qb_recv,
    gx_send, gx_recv, gz_send, gz_recv, w_send, w_recv,
):
    X, Z, C, Y = sizes
    G = X * C
    T, DL = xb.shape
    S = T // Y
    N = head.shape[1]
    O, H = hout_ref.shape
    CW = N // CHUNKS
    D = DL * Y
    tokens = T * X * Z * C
    x, z, c, j = (lax.axis_index(a) for a in (*TOK, "tp"))
    g = x * C + c
    half = Z // 2
    hd = DL // 2

    def at_y(d):
        return {"tp": lax.rem(j + d, Y)}

    def at_xc(e):
        return {"tok_0": lax.rem(x + e // C, X), "tok_2": lax.rem(c + e % C, C)}

    def at_z(d):
        return {"tok_1": lax.rem(z + d, Z)}

    barrier = pltpu.get_barrier_semaphore()
    partners = (
        [at_y(d) for d in range(1, Y)] + [at_xc(e) for e in range(1, G)] + [at_z(d) for d in range(1, Z)]
    )
    for where in partners:
        pl.semaphore_signal(barrier, inc=1, device_id=where, device_id_type=pl.DeviceIdType.MESH)

    def rows_of(group):
        return pl.ds(pl.multiple_of(group * T, T), T)

    mine = rows_of(g)
    load = pltpu.make_async_copy(resid_hbm, resids.at[mine, :], load_sem.at[CHUNKS])
    load.start()
    small = [
        pltpu.make_async_copy(src, dst, small_sem.at[k])
        for k, (src, dst) in enumerate(
            (
                (gain_hbm, gain_ref),
                (bias_hbm, bias_ref),
                (hout_hbm, hout_ref),
                (tgt_hbm, tgt_ref),
                (mask_hbm, mask_ref),
                (ow_hbm, ow_ref),
            )
        )
    ]
    for copy in small:
        copy.start()
    def block_of(d):
        return lax.rem(x + d, X)

    def cols_of(d):
        return pl.ds(pl.multiple_of(block_of(d) * CW, CW), CW)

    head_loads = {
        d: pltpu.make_async_copy(head_hbm.at[:, cols_of(d)], head.at[:, cols_of(d)], load_sem.at[d])
        for d in STEPS
    }
    for d in STEPS:
        head_loads[d].start()
    load.wait()
    pl.semaphore_wait(barrier, len(partners))

    east, west, twin = {"tok_0": lax.rem(x + 1, X)}, {"tok_0": lax.rem(x + X - 1, X)}, {"tok_2": 1 - c}

    def resid_copy(group, first, count, where, k):
        block = resids.at[pl.ds(pl.multiple_of(group * T + first, count), count), :]
        return remote(block, block, r_send.at[k], r_recv.at[k], where)

    g_west = lax.rem(x + X - 1, X) * C + c
    g_east = lax.rem(x + 1, X) * C + c
    g_far = lax.rem(x + 2, X) * C + c
    far = T // 2
    r_copies = [
        resid_copy(g, 0, far, east, 0),
        resid_copy(g, far, far, west, 1),
        resid_copy(g, far, far, east, 2),
        resid_copy(g, 0, far, west, 3),
        resid_copy(g, 0, T, twin, 4),
        resid_copy(g_west, 0, far, east, 5),
        resid_copy(g_east, far, far, west, 6),
        resid_copy(g_west, 0, T, twin, 7),
        resid_copy(g_east, 0, T, twin, 8),
        resid_copy(g_far, 0, T, twin, 9),
    ]

    for k in range(5):
        r_copies[k].start()

    for copy in small:
        copy.wait()
    tgt_t[...] = jnp.transpose(tgt_ref[...])
    mask_t[...] = jnp.transpose(mask_ref[...].astype(F32))
    total = jnp.zeros((T, 128), F32)
    for i in range(DL // 128):
        lanes = slice(i * 128, (i + 1) * 128)
        r = resids[mine, lanes].astype(F32)
        total = total + r * r
        xb[:, lanes] = (r * gain_ref[:, lanes]).astype(BF16)
    sums[...] = total

    def quarter(k):
        return pl.ds(pl.multiple_of(k * S, S), S)

    own = quarter(j)
    s_copies = []
    for k in range(1, Y):
        to = lax.rem(j + k, Y)
        copy = remote(
            sums.at[quarter(to), :], sums_in.at[k - 1], s_send.at[k - 1], s_recv.at[k - 1], at_y(k)
        )
        copy.start()
        s_copies.append(copy)
    y_copies = {}
    for d in STEPS:
        cols = cols_of(d)
        head_loads[d].wait()
        part[:, cols] = jnp.dot(xb[...], head[:, cols], preferred_element_type=F32).astype(BF16)
        y_copies[d] = []
        for k in range(1, Y):
            to = lax.rem(j + k, Y)
            copy = remote(
                part.at[quarter(to), cols],
                parts_in.at[k - 1, :, cols],
                y_send.at[k - 1, d],
                y_recv.at[k - 1, d],
                at_y(k),
            )
            copy.start()
            y_copies[d].append(copy)

    for copy in s_copies:
        copy.wait()
    square = sums[own, :]
    for k in range(Y - 1):
        square = square + sums_in[k]
    inv = lax.rsqrt(jnp.sum(square, axis=1, keepdims=True) / D + norm_eps)
    inverses[own, :] = jnp.broadcast_to(inv, (S, 128))
    i_copies = []
    for k in range(1, Y):
        block = inverses.at[own, :]
        copy = remote(block, block, i_send.at[k - 1], i_recv.at[k - 1], at_y(k))
        copy.start()
        i_copies.append(copy)

    lane = lax.broadcasted_iota(jnp.int32, (S, 128), 1)
    lane_o = lax.broadcasted_iota(jnp.int32, (S, O), 1)
    tgt = tgt_t[own, :]
    mask = mask_t[own, :]
    extra = jnp.zeros((S, 128), F32)
    per = O // CHUNKS

    def lanes_of(d, i):
        return pl.ds(pl.multiple_of(block_of(d) * CW + i * H, H), H)

    ag_copies = {}
    for d in STEPS:
        for copy in y_copies[d]:
            copy.wait()
        for i in range(per):
            lanes = lanes_of(d, i)
            o = block_of(d) * per + i
            value = part[own, lanes].astype(F32)
            for k in range(Y - 1):
                value = value + parts_in[k, :, lanes].astype(F32)
            value = value * inv
            cube = value + bias_ref[:, lanes]
            out = hout_ref[pl.ds(o, 1), :]
            squash = jax.nn.sigmoid(cube)
            score = jnp.sum(cube * squash * out, axis=1, keepdims=True)
            here = lane_o == o
            label = jnp.sum(jnp.where(here, mask, 0.0), axis=1, keepdims=True)
            target = jnp.sum(jnp.where(here, tgt, 0.0), axis=1, keepdims=True)
            error = label * (score - target)
            grad = (error * out * (squash * (1.0 + cube * (1.0 - squash)))).astype(BF16)
            rg[own, lanes] = grad
            moment = jnp.sum(grad.astype(F32) * value, axis=1, keepdims=True)
            extra = jnp.where(lane == o, moment, extra)
        ag_copies[d] = []
        for k in range(1, Y):
            block = rg.at[own, cols_of(d)]
            copy = remote(block, block, ag_send.at[k - 1, d], ag_recv.at[k - 1, d], at_y(k))
            copy.start()
            ag_copies[d].append(copy)
    aux[own, :] = extra
    a_copies = []
    for k in range(1, Y):
        block = aux.at[own, :]
        copy = remote(block, block, a_send.at[k - 1], a_recv.at[k - 1], at_y(k))
        copy.start()
        a_copies.append(copy)

    r_copies[0].wait_recv()
    r_copies[5].start()
    r_copies[1].wait_recv()
    r_copies[6].start()

    step = 512

    def objective(d, i, carry):
        lanes = lanes_of(d, i)
        o = block_of(d) * per + i
        lhs = rg[:, lanes]
        total = jnp.zeros((8, 128), F32)
        for k in range(DL // step):
            v = lax.dot_general(
                lhs,
                head[k * step : (k + 1) * step, lanes],
                (((1,), (1,)), ((), ())),
                preferred_element_type=F32,
            )
            vals[o, :, k * step : (k + 1) * step] = v
            for q in range(step // 128):
                w = v[:, q * 128 : (q + 1) * 128]
                total = total + jnp.sum((w * w).reshape(T // 8, 8, 128), axis=0)
        sqp[o] = total
        return carry

    for copy in i_copies:
        copy.wait()
    t_copies = []
    for d in STEPS:
        for copy in ag_copies[d]:
            copy.wait()
        for i in range(per):
            scaled = rg[:, lanes_of(d, i)].astype(F32) * inverses[...]
            flipped = jnp.transpose(scaled).astype(BF16)
            for b in range(H // 32):
                k = i * (H // 32) + b
                grad_t[d, k // C, k % C] = flipped[b * 32 : (b + 1) * 32, :]
        for e in range(d * C, (d + 1) * C):
            where = at_xc(e)
            if e == 0:
                grads[g] = grad_t[0, :, c]
                continue
            copy = remote(
                grad_t.at[d, :, where["tok_2"]],
                grads.at[g],
                t_send.at[e - 1],
                t_recv.at[e - 1],
                where,
            )
            copy.start()
            t_copies.append(copy)
        lax.fori_loop(0, per, functools.partial(objective, d), 0)

    eye = lax.broadcasted_iota(jnp.int32, (O, 128), 0) == lax.broadcasted_iota(jnp.int32, (O, 128), 1)
    local = jnp.sum(jnp.sum(sqp[...], axis=1), axis=1, keepdims=True)
    msg_y[j] = jnp.broadcast_to(jnp.sum(jnp.where(eye, local, 0.0), axis=0, keepdims=True), (8, 128))
    qy = []
    for d in range(1, Y):
        copy = remote(msg_y.at[j], msg_y.at[j], qy_send.at[d - 1], qy_recv.at[d - 1], at_y(d))
        copy.start()
        qy.append(copy)
    share_o = O // Y
    rows8 = lax.broadcasted_iota(jnp.int32, (8, 128), 0)
    bias_rows = jnp.zeros((8, 128), F32)
    for k in range(share_o):
        lanes = pl.ds(pl.multiple_of((j * share_o + k) * H, H), H)
        line = jnp.sum(rg[:, lanes].astype(F32), axis=0, keepdims=True)
        bias_rows = jnp.where(rows8 == k + 1, line, bias_rows)

    r_copies[2].wait_recv()
    r_copies[7].start()
    r_copies[3].wait_recv()
    r_copies[8].start()
    for copy in qy:
        copy.wait()
    squares = msg_y[0]
    for k in range(1, Y):
        squares = squares + msg_y[k]
    msg_z[z] = jnp.where(rows8 == 0, squares, bias_rows)
    qz = []
    for k in range(1, Z):
        copy = remote(msg_z.at[z], msg_z.at[z], qz_send.at[k - 1], qz_recv.at[k - 1], at_z(k))
        copy.start()
        qz.append(copy)
    r_copies[5].wait_recv()
    r_copies[6].wait_recv()
    r_copies[9].start()
    for copy in a_copies:
        copy.wait()
    for copy in qz:
        copy.wait()
    both = msg_z[0]
    for k in range(1, Z):
        both = both + msg_z[k]
    msg_x[g] = both
    qx = []
    for e in range(1, G):
        copy = remote(msg_x.at[g], msg_x.at[g], qx_send.at[e - 1], qx_recv.at[e - 1], at_xc(e))
        copy.start()
        qx.append(copy)
    for k in (4, 7, 8, 9):
        r_copies[k].wait_recv()
    for copy in t_copies:
        copy.wait()

    wstep = 256

    def weight(i, carry):
        lanes = pl.ds(pl.multiple_of(i * wstep, wstep), wstep)
        lhs = jnp.concatenate([grads[k].reshape(Z * 32, T) for k in range(G)], axis=1)
        v = jnp.dot(lhs, resids[:, lanes], preferred_element_type=F32)
        wt[:, :, lanes] = v.reshape(Z, 32, wstep)
        return carry

    chains = ((0, 1, half), (1, -1, half), (1, 1, half - 1), (0, -1, half - 1))
    base = (0, half, 2 * half, 3 * half - 1)

    def chain_copy(k, s):
        _, direction, _ = chains[k]
        slot = base[k] + s
        return remote(
            stage.at[slot],
            inbox.at[slot],
            w_send.at[slot],
            w_recv.at[slot],
            at_z(1 if direction > 0 else Z - 1),
        )

    def chain_step(k, s):
        part_of, direction, count = chains[k]
        distance = count - s
        owner = lax.rem(z + (distance if direction > 0 else Z - distance), Z)
        lanes = slice(part_of * hd, (part_of + 1) * hd)
        value = wt[owner, :, lanes]
        if s > 0:
            chain_copy(k, s - 1).wait_recv()
            value = value + inbox[base[k] + s - 1].astype(F32)
        stage[base[k] + s] = value.astype(BF16)
        chain_copy(k, s).start()

    lax.fori_loop(0, hd // wstep, weight, 0)
    chain_step(0, 0)
    chain_step(3, 0)

    lax.fori_loop(hd // wstep, DL // wstep, weight, 0)
    chain_step(1, 0)
    chain_step(2, 0)

    def round_of(s, which=(0, 3, 1, 2)):
        for k in which:
            if s < chains[k][2]:
                chain_step(k, s)

    for copy in qx:
        copy.wait()
    both = msg_x[0]
    for k in range(1, G):
        both = both + msg_x[k]
    msg_b[j] = both
    qb = []
    for d in range(1, Y):
        copy = remote(msg_b.at[j], msg_b.at[j], qb_send.at[d - 1], qb_recv.at[d - 1], at_y(d))
        copy.start()
        qb.append(copy)
    eye16 = lax.broadcasted_iota(jnp.int32, (O, O), 0) == lax.broadcasted_iota(jnp.int32, (O, O), 1)
    squares = jnp.sum(jnp.where(eye, both[0:1, :], 0.0), axis=1, keepdims=True)
    weights = jnp.sum(jnp.where(eye16, ow_ref[...].astype(F32), 0.0), axis=1, keepdims=True)
    balance = weights / denominator / jnp.sqrt(squares / (tokens * D) + grad_eps)
    balance_row = jnp.sum(jnp.where(eye, balance, 0.0), axis=0, keepdims=True)

    inverse = inverses[...]
    projection = jnp.sum(
        jnp.where(lax.broadcasted_iota(jnp.int32, (T, 128), 1) < O, aux[...] * balance_row, 0.0),
        axis=1,
        keepdims=True,
    )
    shrink = projection / D
    factors = [jnp.broadcast_to(balance[o : o + 1, :], (8, 128)) for o in range(O)]

    def combine(i, carry):
        lanes = pl.ds(pl.multiple_of(i * 128, 128), 128)
        norm = jnp.zeros((T // 8, 8, 128), F32)
        for o in range(O):
            norm = norm + vals[o, :, lanes].reshape(T // 8, 8, 128) * factors[o][None]
        norm = norm.reshape(T, 128)
        unit = resids[mine, lanes].astype(F32) * inverse
        gpart[i] = jnp.sum((norm * unit).reshape(T // 8, 8, 128), axis=0)
        dx_ref[:, lanes] = (inverse * (gain_ref[:, lanes] * norm - unit * shrink)).astype(BF16)
        return carry

    pieces = DL // 128
    lax.fori_loop(0, pieces // 2, combine, 0)
    if half > 1:
        round_of(1, (0, 3))
    lax.fori_loop(pieces // 2, pieces, combine, 0)
    gmsg[...] = jnp.sum(gpart[...], axis=1)
    gmsg_x[g] = gmsg[...]
    gx = []
    for e in range(1, G):
        copy = remote(gmsg, gmsg_x.at[g], gx_send.at[e - 1], gx_recv.at[e - 1], at_xc(e))
        copy.start()
        gx.append(copy)
    if half > 1:
        round_of(1, (1, 2))
    if half > 2:
        round_of(2)
    for copy in gx:
        copy.wait()
    both = gmsg_x[0]
    for k in range(1, G):
        both = both + gmsg_x[k]
    gmsg_z[z] = both
    gz = []
    for d in range(1, Z):
        copy = remote(gmsg_z.at[z], gmsg_z.at[z], gz_send.at[d - 1], gz_recv.at[d - 1], at_z(d))
        copy.start()
        gz.append(copy)

    for s in range(3, half):
        round_of(s)

    k_own = (x * Z + z) * C + c
    objective_own = k_own * 32 // H
    scale = jnp.sum(
        jnp.where(lax.broadcasted_iota(jnp.int32, (O, 1), 0) == objective_own, balance, 0.0),
        axis=0,
        keepdims=True,
    )
    for part_of in range(2):
        lanes = slice(part_of * hd, (part_of + 1) * hd)
        value = wt[z, :, lanes]
        for k in range(4):
            if chains[k][0] == part_of and chains[k][2] > 0:
                chain_copy(k, chains[k][2] - 1).wait_recv()
                value = value + inbox[base[k] + chains[k][2] - 1].astype(F32)
        wg_ref[:, lanes] = value * gain_ref[:, lanes] * scale / tokens

    for copy in qb:
        copy.wait()
    for k in range(Y):
        for i in range(share_o):
            o = k * share_o + i
            bg_ref[o : o + 1, :] = msg_b[k, i + 1 : i + 2, :] * balance[o : o + 1, :] / tokens
    for copy in gz:
        copy.wait()
    both = gmsg_z[0]
    for k in range(1, Z):
        both = both + gmsg_z[k]
    gg_ref[...] = both / tokens

    for copy in r_copies:
        copy.wait_send()
    for k in range(4):
        for s in range(chains[k][2]):
            chain_copy(k, s).wait_send()


def settle(dx_ref, gg_ref, wg_ref, bg_ref, dx_out, gg_out, wg_out, bg_out):
    dx_out[...] = dx_ref[...]
    gg_out[...] = gg_ref[...]
    wg_out[...] = wg_ref[...]
    bg_out[...] = bg_ref[...]


def per_device(resid, norm_gain, head_in, head_bias, head_out, targets, label_mask, obj_weight):
    X, Z, C, Y = (lax.axis_size(a) for a in (*TOK, "tp"))
    G = X * C
    T, DL = resid.shape
    N = head_in.shape[1]
    O, H = head_out.shape
    S = T // Y
    CW = N // CHUNKS
    columns = N // (X * Z * C)
    slots = 2 * (Z - 1)
    hbm = pl.BlockSpec(memory_space=pltpu.HBM)
    vmem = pl.BlockSpec(memory_space=pltpu.VMEM)
    dma = pltpu.SemaphoreType.DMA
    V = pltpu.VMEM
    scratch = [
        V((1, DL), F32),
        V((1, N), F32),
        V((O, H), F32),
        V((O, T), F32),
        V((O, T), jnp.int32),
        V((1, O), jnp.int32),
        V((T, O), F32),
        V((T, O), F32),
        V((G * T, DL), BF16),
        V((DL, N), BF16),
        V((T, DL), BF16),
        V((T, N), BF16),
        V((Y - 1, S, N), BF16),
        V((T, 128), F32),
        V((Y - 1, S, 128), F32),
        V((T, N), BF16),
        V((T, 128), F32),
        V((T, 128), F32),
        V((X, Z, C, columns, T), BF16),
        V((G, Z, columns, T), BF16),
        V((O, T, DL), F32),
        V((O, 8, 128), F32),
        V((Y, 8, 128), F32),
        V((Y, 8, 128), F32),
        V((G, 8, 128), F32),
        V((Z, 8, 128), F32),
        V((DL // 128, 8, 128), F32),
        V((DL // 128, 128), F32),
        V((G, DL // 128, 128), F32),
        V((Z, DL // 128, 128), F32),
        V((Z, columns, DL), F32),
        V((slots, columns, DL // 2), BF16),
        V((slots, columns, DL // 2), BF16),
        dma((CHUNKS + 1,)), dma((6,)),
        dma((Y - 1, CHUNKS)), dma((Y - 1, CHUNKS)),
        dma((Y - 1,)), dma((Y - 1,)),
        dma((Y - 1, CHUNKS)), dma((Y - 1, CHUNKS)),
        dma((Y - 1,)), dma((Y - 1,)),
        dma((Y - 1,)), dma((Y - 1,)),
        dma((10,)), dma((10,)),
        dma((G - 1,)), dma((G - 1,)),
        dma((Y - 1,)), dma((Y - 1,)),
        dma((G - 1,)), dma((G - 1,)),
        dma((Z - 1,)), dma((Z - 1,)),
        dma((Y - 1,)), dma((Y - 1,)),
        dma((G - 1,)), dma((G - 1,)),
        dma((Z - 1,)), dma((Z - 1,)),
        dma((slots,)), dma((slots,)),
    ]
    dx, gg, wg, bg = pl.pallas_call(
        functools.partial(kernel, (X, Z, C, Y)),
        out_shape=(
            jax.ShapeDtypeStruct((T, DL), BF16),
            jax.ShapeDtypeStruct((DL // 128, 128), F32),
            jax.ShapeDtypeStruct((columns, DL), F32),
            jax.ShapeDtypeStruct((O, H), F32),
        ),
        in_specs=[hbm] * 8,
        out_specs=(vmem,) * 4,
        scratch_shapes=scratch,
        compiler_params=pltpu.CompilerParams(
            collective_id=0, has_side_effects=True, vmem_limit_bytes=48 << 20
        ),
    )(
        *(
            pltpu.with_memory_space_constraint(a, pltpu.HBM)
            for a in (
                resid,
                head_in,
                norm_gain.reshape(1, DL),
                head_bias.reshape(1, N),
                head_out,
                targets.T,
                label_mask.T,
                obj_weight.reshape(1, O),
            )
        )
    )
    dx, gg, wg, bg = pl.pallas_call(
        settle,
        out_shape=tuple(jax.ShapeDtypeStruct(a.shape, a.dtype) for a in (dx, gg, wg, bg)),
        in_specs=[vmem] * 4,
        out_specs=(vmem,) * 4,
        compiler_params=pltpu.CompilerParams(vmem_limit_bytes=4 << 20),
    )(dx, gg, wg, bg)
    return dx, gg.reshape(DL), wg.T, bg.reshape(N)


def solution(mesh):
    finer = Mesh(mesh.devices.reshape(4, 8, 2, mesh.shape["tp"]), ("tok_0", "tok_1", "tok_2", "tp"))
    placed = (P(TOK, "tp"), P("tp"), P("tp", None), P(), P(), P(TOK, None), P(TOK, None), P())
    return jax.shard_map(
        per_device,
        mesh=finer,
        in_specs=placed,
        out_specs=(P(TOK, "tp"), P("tp"), P("tp", TOK), P()),
        check_vma=False,
    )
```

```python
import functools

import jax
import jax.numpy as jnp
from jax import lax
from jax.experimental import pallas as pl
from jax.experimental.pallas import tpu as pltpu
from jax.sharding import Mesh
from jax.sharding import PartitionSpec as P

TOK = ("tok_0", "tok_1", "tok_2")
F32 = jnp.float32
BF16 = jnp.bfloat16

norm_eps = 1e-05
grad_eps = 1e-06
denominator = 8.0

STEPS = (2, 1, 3, 0)
CHUNKS = len(STEPS)
PARTS = 4


def remote(src, dst, send, recv, where):
    return pltpu.make_async_remote_copy(
        src_ref=src,
        dst_ref=dst,
        send_sem=send,
        recv_sem=recv,
        device_id=where,
        device_id_type=pl.DeviceIdType.MESH,
    )


def kernel(
    sizes,
    resid_hbm, head_hbm, gain_hbm, bias_hbm, hout_hbm, tgt_hbm, mask_hbm, ow_hbm,
    dx_ref, gg_ref, wg_ref, bg_ref,
    gain_ref, bias_ref, hout_ref, tgt_ref, mask_ref, ow_ref,
    tgt_t, mask_t, resids, head, xb, part, parts_in, sums, sums_in, rg, aux, inverses, grad_t, grads, vals, sqp,
    msg_b, msg_p, msg_x, msg_z, gpart, gmsg, gmsg_x, gmsg_z, wt, stage, inbox,
    load_sem, small_sem, y_send, y_recv, s_send, s_recv, ag_send, ag_recv, a_send, a_recv, i_send, i_recv,
    r_send, r_recv, t_send, t_recv, qp_send, qp_recv, qx_send, qx_recv, qz_send, qz_recv, qb_send, qb_recv,
    gx_send, gx_recv, gz_send, gz_recv, w_send, w_recv,
):
    X, Z, C, Y = sizes
    G = X * C
    T, DL = xb.shape
    S = T // Y
    N = head.shape[1]
    O, H = hout_ref.shape
    CW = N // CHUNKS
    D = DL * Y
    tokens = T * X * Z * C
    x, z, c, j = (lax.axis_index(a) for a in (*TOK, "tp"))
    g = x * C + c
    half = Z // 2
    hd = DL // PARTS

    def at_y(d):
        return {"tp": lax.rem(j + d, Y)}

    def at_xc(e):
        return {"tok_0": lax.rem(x + e // C, X), "tok_2": lax.rem(c + e % C, C)}

    def at_z(d):
        return {"tok_1": lax.rem(z + d, Z)}

    def rows_of(group):
        return pl.ds(pl.multiple_of(group * T, T), T)

    mine = rows_of(g)
    load = pltpu.make_async_copy(resid_hbm, resids.at[mine, :], load_sem.at[CHUNKS])
    load.start()
    small = [
        pltpu.make_async_copy(src, dst, small_sem.at[k])
        for k, (src, dst) in enumerate(
            (
                (gain_hbm, gain_ref),
                (bias_hbm, bias_ref),
                (hout_hbm, hout_ref),
                (tgt_hbm, tgt_ref),
                (mask_hbm, mask_ref),
                (ow_hbm, ow_ref),
            )
        )
    ]
    small[0].start()
    for copy in small[1:]:
        copy.start(priority=1)
    def block_of(d):
        return lax.rem(x + d, X)

    def cols_of(d):
        return pl.ds(pl.multiple_of(block_of(d) * CW, CW), CW)

    head_loads = {
        d: pltpu.make_async_copy(head_hbm.at[:, cols_of(d)], head.at[:, cols_of(d)], load_sem.at[d])
        for d in STEPS
    }
    for d in STEPS:
        head_loads[d].start()

    def at_plane(k):
        return {**at_y(k // G), **at_xc(k % G)}

    barrier = pltpu.get_barrier_semaphore()
    partners = [at_plane(k) for k in range(1, Y * G)] + [at_z(d) for d in range(1, Z)]
    for where in partners:
        pl.semaphore_signal(barrier, inc=1, device_id=where, device_id_type=pl.DeviceIdType.MESH)

    load.wait()
    pl.semaphore_wait(barrier, len(partners))

    east, west, twin = {"tok_0": lax.rem(x + 1, X)}, {"tok_0": lax.rem(x + X - 1, X)}, {"tok_2": 1 - c}

    def resid_copy(group, first, count, where, k):
        block = resids.at[pl.ds(pl.multiple_of(group * T + first, count), count), :]
        return remote(block, block, r_send.at[k], r_recv.at[k], where)

    g_west = lax.rem(x + X - 1, X) * C + c
    g_east = lax.rem(x + 1, X) * C + c
    g_far = lax.rem(x + 2, X) * C + c
    far = T // 2
    r_copies = [
        resid_copy(g, 0, far, east, 0),
        resid_copy(g, far, far, west, 1),
        resid_copy(g, far, far, east, 2),
        resid_copy(g, 0, far, west, 3),
        resid_copy(g, 0, T, twin, 4),
        resid_copy(g_west, 0, far, east, 5),
        resid_copy(g_east, far, far, west, 6),
        resid_copy(g_west, 0, T, twin, 7),
        resid_copy(g_east, 0, T, twin, 8),
        resid_copy(g_far, 0, T, twin, 9),
    ]

    for k in range(5):
        r_copies[k].start()

    small[0].wait()
    total = jnp.zeros((T, 128), F32)
    for i in range(DL // 128):
        lanes = slice(i * 128, (i + 1) * 128)
        r = resids[mine, lanes].astype(F32)
        total = total + r * r
        xb[:, lanes] = (r * gain_ref[:, lanes]).astype(BF16)
    sums[...] = total

    def quarter(k):
        return pl.ds(pl.multiple_of(k * S, S), S)

    own = quarter(j)
    s_copies = []
    for k in range(1, Y):
        to = lax.rem(j + k, Y)
        copy = remote(
            sums.at[quarter(to), :], sums_in.at[k - 1], s_send.at[k - 1], s_recv.at[k - 1], at_y(k)
        )
        copy.start()
        s_copies.append(copy)
    y_copies = {}
    for d in STEPS:
        cols = cols_of(d)
        head_loads[d].wait()
        part[:, cols] = jnp.dot(xb[...], head[:, cols], preferred_element_type=F32).astype(BF16)
        y_copies[d] = []
        for k in range(1, Y):
            to = lax.rem(j + k, Y)
            copy = remote(
                part.at[quarter(to), cols],
                parts_in.at[k - 1, :, cols],
                y_send.at[k - 1, d],
                y_recv.at[k - 1, d],
                at_y(k),
            )
            copy.start()
            y_copies[d].append(copy)

    for copy in small[1:]:
        copy.wait()
    tgt_t[...] = jnp.transpose(tgt_ref[...])
    mask_t[...] = jnp.transpose(mask_ref[...].astype(F32))
    for copy in s_copies:
        copy.wait()
    square = sums[own, :]
    for k in range(Y - 1):
        square = square + sums_in[k]
    inv = lax.rsqrt(jnp.sum(square, axis=1, keepdims=True) / D + norm_eps)
    inverses[own, :] = jnp.broadcast_to(inv, (S, 128))
    i_copies = []
    for k in range(1, Y):
        block = inverses.at[own, :]
        copy = remote(block, block, i_send.at[k - 1], i_recv.at[k - 1], at_y(k))
        copy.start()
        i_copies.append(copy)

    lane = lax.broadcasted_iota(jnp.int32, (S, 128), 1)
    lane_o = lax.broadcasted_iota(jnp.int32, (S, O), 1)
    tgt = tgt_t[own, :]
    mask = mask_t[own, :]
    extra = jnp.zeros((S, 128), F32)
    per = O // CHUNKS

    def lanes_of(d, i):
        return pl.ds(pl.multiple_of(block_of(d) * CW + i * H, H), H)

    ag_copies = {}
    for d in STEPS:
        for copy in y_copies[d]:
            copy.wait()
        for i in range(per):
            lanes = lanes_of(d, i)
            o = block_of(d) * per + i
            value = part[own, lanes].astype(F32)
            for k in range(Y - 1):
                value = value + parts_in[k, :, lanes].astype(F32)
            value = value * inv
            cube = value + bias_ref[:, lanes]
            out = hout_ref[pl.ds(o, 1), :]
            squash = jax.nn.sigmoid(cube)
            score = jnp.sum(cube * squash * out, axis=1, keepdims=True)
            here = lane_o == o
            label = jnp.sum(jnp.where(here, mask, 0.0), axis=1, keepdims=True)
            target = jnp.sum(jnp.where(here, tgt, 0.0), axis=1, keepdims=True)
            error = label * (score - target)
            grad = (error * out * (squash * (1.0 + cube * (1.0 - squash)))).astype(BF16)
            rg[own, lanes] = grad
            moment = jnp.sum(grad.astype(F32) * value, axis=1, keepdims=True)
            extra = jnp.where(lane == o, moment, extra)
        ag_copies[d] = []
        for k in range(1, Y):
            block = rg.at[own, cols_of(d)]
            copy = remote(block, block, ag_send.at[k - 1, d], ag_recv.at[k - 1, d], at_y(k))
            copy.start()
            ag_copies[d].append(copy)
    aux[own, :] = extra
    a_copies = []
    for k in range(1, Y):
        block = aux.at[own, :]
        copy = remote(block, block, a_send.at[k - 1], a_recv.at[k - 1], at_y(k))
        copy.start()
        a_copies.append(copy)

    r_copies[0].wait_recv()
    r_copies[5].start()
    r_copies[1].wait_recv()
    r_copies[6].start()

    step = 512

    def objective(d, i, carry):
        lanes = lanes_of(d, i)
        o = block_of(d) * per + i
        lhs = rg[:, lanes]
        total = jnp.zeros((8, 128), F32)
        for k in range(DL // step):
            v = lax.dot_general(
                lhs,
                head[k * step : (k + 1) * step, lanes],
                (((1,), (1,)), ((), ())),
                preferred_element_type=F32,
            )
            vals[o, :, k * step : (k + 1) * step] = v
            for q in range(step // 128):
                w = v[:, q * 128 : (q + 1) * 128]
                total = total + jnp.sum((w * w).reshape(T // 8, 8, 128), axis=0)
        sqp[o] = total
        return carry

    for copy in i_copies:
        copy.wait()
    t_copies = []
    for d in STEPS:
        for copy in ag_copies[d]:
            copy.wait()
        for i in range(per):
            scaled = rg[:, lanes_of(d, i)].astype(F32) * inverses[...]
            flipped = jnp.transpose(scaled).astype(BF16)
            for b in range(H // 32):
                k = i * (H // 32) + b
                grad_t[d, k // C, k % C] = flipped[b * 32 : (b + 1) * 32, :]
        for e in range(d * C, (d + 1) * C):
            where = at_xc(e)
            if e == 0:
                grads[g] = grad_t[0, :, c]
                continue
            copy = remote(
                grad_t.at[d, :, where["tok_2"]],
                grads.at[g],
                t_send.at[e - 1],
                t_recv.at[e - 1],
                where,
            )
            copy.start()
            t_copies.append(copy)
        lax.fori_loop(0, per, functools.partial(objective, d), 0)

    eye = lax.broadcasted_iota(jnp.int32, (O, 128), 0) == lax.broadcasted_iota(jnp.int32, (O, 128), 1)
    local = jnp.sum(jnp.sum(sqp[...], axis=1), axis=1, keepdims=True)
    squares = jnp.sum(jnp.where(eye, local, 0.0), axis=0, keepdims=True)
    share_o = O // Y
    rows8 = lax.broadcasted_iota(jnp.int32, (8, 128), 0)
    bias_rows = jnp.zeros((8, 128), F32)
    for k in range(share_o):
        lanes = pl.ds(pl.multiple_of((j * share_o + k) * H, H), H)
        line = jnp.sum(rg[:, lanes].astype(F32), axis=0, keepdims=True)
        bias_rows = jnp.where(rows8 == k + 1, line, bias_rows)

    msg_z[z] = jnp.where(rows8 == 0, squares, bias_rows)
    qz = []
    for k in range(1, Z):
        copy = remote(msg_z.at[z], msg_z.at[z], qz_send.at[k - 1], qz_recv.at[k - 1], at_z(k))
        copy.start()
        qz.append(copy)

    r_copies[2].wait_recv()
    r_copies[7].start()
    r_copies[3].wait_recv()
    r_copies[8].start()
    r_copies[5].wait_recv()
    r_copies[6].wait_recv()
    r_copies[9].start()
    for copy in a_copies:
        copy.wait()
    for copy in qz:
        copy.wait()
    both = msg_z[0]
    for k in range(1, Z):
        both = both + msg_z[k]
    seat = j * G + g
    msg_p[seat] = both[0:1, :]
    msg_x[g] = both
    qp = []
    for k in range(1, Y * G):
        copy = remote(msg_p.at[seat], msg_p.at[seat], qp_send.at[k - 1], qp_recv.at[k - 1], at_plane(k))
        copy.start()
        qp.append(copy)
    qx = []
    for e in range(1, G):
        copy = remote(msg_x.at[g], msg_x.at[g], qx_send.at[e - 1], qx_recv.at[e - 1], at_xc(e))
        copy.start()
        qx.append(copy)
    for k in (4, 7, 8, 9):
        r_copies[k].wait_recv()
    for copy in t_copies:
        copy.wait_recv()

    def weight(p):
        lanes = slice(p * hd, (p + 1) * hd)
        lhs = jnp.concatenate([grads[k].reshape(Z * 32, T) for k in range(G)], axis=1)
        v = jnp.dot(lhs, resids[:, lanes], preferred_element_type=F32)
        wt[:, :, lanes] = v.reshape(Z, 32, hd)

    def count_of(p, way):
        return half - (p + way) % 2

    def slot_of(p, way, s):
        return (p * (2 * half - 1)) + (half - p % 2 if way else 0) + s

    def chain_copy(p, way, s):
        slot = slot_of(p, way, s)
        return remote(
            stage.at[slot],
            inbox.at[slot],
            w_send.at[slot],
            w_recv.at[slot],
            at_z(Z - 1 if way else 1),
        )

    def chain_step(p, s):
        lanes = slice(p * hd, (p + 1) * hd)
        for way in range(2):
            count = count_of(p, way)
            if s < count:
                distance = count - s
                owner = lax.rem(z + (Z - distance if way else distance), Z)
                value = wt[owner, :, lanes]
                if s > 0:
                    chain_copy(p, way, s - 1).wait_recv()
                    value = value + inbox[slot_of(p, way, s - 1)].astype(F32)
                stage[slot_of(p, way, s)] = value.astype(BF16)
                chain_copy(p, way, s).start()

    for p in range(PARTS):
        weight(p)
        chain_step(p, 0)
    for copy in qp:
        copy.wait()
    squares = msg_p[0]
    for k in range(1, Y * G):
        squares = squares + msg_p[k]
    eye16 = lax.broadcasted_iota(jnp.int32, (O, O), 0) == lax.broadcasted_iota(jnp.int32, (O, O), 1)
    squares = jnp.sum(jnp.where(eye, squares, 0.0), axis=1, keepdims=True)
    weights = jnp.sum(jnp.where(eye16, ow_ref[...].astype(F32), 0.0), axis=1, keepdims=True)
    balance = weights / denominator / jnp.sqrt(squares / (tokens * D) + grad_eps)
    balance_row = jnp.sum(jnp.where(eye, balance, 0.0), axis=0, keepdims=True)

    inverse = inverses[...]
    projection = jnp.sum(
        jnp.where(lax.broadcasted_iota(jnp.int32, (T, 128), 1) < O, aux[...] * balance_row, 0.0),
        axis=1,
        keepdims=True,
    )
    shrink = projection / D
    factors = [jnp.broadcast_to(balance[o : o + 1, :], (8, 128)) for o in range(O)]

    def combine(i, carry):
        lanes = pl.ds(pl.multiple_of(i * 128, 128), 128)
        norm = jnp.zeros((T // 8, 8, 128), F32)
        for o in range(O):
            norm = norm + vals[o, :, lanes].reshape(T // 8, 8, 128) * factors[o][None]
        norm = norm.reshape(T, 128)
        unit = resids[mine, lanes].astype(F32) * inverse
        gpart[i] = jnp.sum((norm * unit).reshape(T // 8, 8, 128), axis=0)
        dx_ref[:, lanes] = (inverse * (gain_ref[:, lanes] * norm - unit * shrink)).astype(BF16)
        return carry

    pieces = DL // 128
    for p in range(PARTS):
        lax.fori_loop(p * pieces // PARTS, (p + 1) * pieces // PARTS, combine, 0)
        if half > 1:
            chain_step(p, 1)
    gmsg[...] = jnp.sum(gpart[...], axis=1)
    gmsg_x[g] = gmsg[...]
    gx = []
    for e in range(1, G):
        copy = remote(gmsg, gmsg_x.at[g], gx_send.at[e - 1], gx_recv.at[e - 1], at_xc(e))
        copy.start()
        gx.append(copy)
    if half > 2:
        for p in range(PARTS):
            chain_step(p, 2)
    for copy in qx:
        copy.wait()
    both = msg_x[0]
    for k in range(1, G):
        both = both + msg_x[k]
    msg_b[j] = both
    qb = []
    for k in range(1, Y):
        copy = remote(msg_b.at[j], msg_b.at[j], qb_send.at[k - 1], qb_recv.at[k - 1], at_y(k))
        copy.start()
        qb.append(copy)
    for copy in gx:
        copy.wait()
    both = gmsg_x[0]
    for k in range(1, G):
        both = both + gmsg_x[k]
    gmsg_z[z] = both
    gz = []
    for d in range(1, Z):
        copy = remote(gmsg_z.at[z], gmsg_z.at[z], gz_send.at[d - 1], gz_recv.at[d - 1], at_z(d))
        copy.start()
        gz.append(copy)

    for s in range(3, half):
        for p in range(PARTS):
            chain_step(p, s)

    k_own = (x * Z + z) * C + c
    objective_own = k_own * 32 // H
    scale = jnp.sum(
        jnp.where(lax.broadcasted_iota(jnp.int32, (O, 1), 0) == objective_own, balance, 0.0),
        axis=0,
        keepdims=True,
    )
    for p in range(PARTS):
        lanes = slice(p * hd, (p + 1) * hd)
        value = wt[z, :, lanes]
        for way in range(2):
            count = count_of(p, way)
            if count > 0:
                chain_copy(p, way, count - 1).wait_recv()
                value = value + inbox[slot_of(p, way, count - 1)].astype(F32)
        wg_ref[:, lanes] = value * gain_ref[:, lanes] * scale / tokens
    for copy in qb:
        copy.wait()
    for k in range(Y):
        for i in range(share_o):
            o = k * share_o + i
            bg_ref[o : o + 1, :] = msg_b[k, i + 1 : i + 2, :] * balance[o : o + 1, :] / tokens
    for copy in gz:
        copy.wait()
    both = gmsg_z[0]
    for k in range(1, Z):
        both = both + gmsg_z[k]
    gg_ref[...] = both / tokens

    for copy in r_copies + t_copies:
        copy.wait_send()
    for p in range(PARTS):
        for way in range(2):
            for s in range(count_of(p, way)):
                chain_copy(p, way, s).wait_send()


def settle(dx_ref, gg_ref, wg_ref, bg_ref, dx_out, gg_out, wg_out, bg_out):
    dx_out[...] = dx_ref[...]
    gg_out[...] = gg_ref[...]
    wg_out[...] = wg_ref[...]
    bg_out[...] = bg_ref[...]


def per_device(resid, norm_gain, head_in, head_bias, head_out, targets, label_mask, obj_weight):
    X, Z, C, Y = (lax.axis_size(a) for a in (*TOK, "tp"))
    G = X * C
    T, DL = resid.shape
    N = head_in.shape[1]
    O, H = head_out.shape
    S = T // Y
    CW = N // CHUNKS
    columns = N // (X * Z * C)
    slots = PARTS * (Z - 1)
    hbm = pl.BlockSpec(memory_space=pltpu.HBM)
    vmem = pl.BlockSpec(memory_space=pltpu.VMEM)
    dma = pltpu.SemaphoreType.DMA
    V = pltpu.VMEM
    scratch = [
        V((1, DL), F32),
        V((1, N), F32),
        V((O, H), F32),
        V((O, T), F32),
        V((O, T), jnp.int32),
        V((1, O), jnp.int32),
        V((T, O), F32),
        V((T, O), F32),
        V((G * T, DL), BF16),
        V((DL, N), BF16),
        V((T, DL), BF16),
        V((T, N), BF16),
        V((Y - 1, S, N), BF16),
        V((T, 128), F32),
        V((Y - 1, S, 128), F32),
        V((T, N), BF16),
        V((T, 128), F32),
        V((T, 128), F32),
        V((X, Z, C, columns, T), BF16),
        V((G, Z, columns, T), BF16),
        V((O, T, DL), F32),
        V((O, 8, 128), F32),
        V((Y, 8, 128), F32),
        V((Y * G, 1, 128), F32),
        V((G, 8, 128), F32),
        V((Z, 8, 128), F32),
        V((DL // 128, 8, 128), F32),
        V((DL // 128, 128), F32),
        V((G, DL // 128, 128), F32),
        V((Z, DL // 128, 128), F32),
        V((Z, columns, DL), F32),
        V((slots, columns, DL // PARTS), BF16),
        V((slots, columns, DL // PARTS), BF16),
        dma((CHUNKS + 1,)), dma((6,)),
        dma((Y - 1, CHUNKS)), dma((Y - 1, CHUNKS)),
        dma((Y - 1,)), dma((Y - 1,)),
        dma((Y - 1, CHUNKS)), dma((Y - 1, CHUNKS)),
        dma((Y - 1,)), dma((Y - 1,)),
        dma((Y - 1,)), dma((Y - 1,)),
        dma((10,)), dma((10,)),
        dma((G - 1,)), dma((G - 1,)),
        dma((Y * G - 1,)), dma((Y * G - 1,)),
        dma((G - 1,)), dma((G - 1,)),
        dma((Z - 1,)), dma((Z - 1,)),
        dma((Y - 1,)), dma((Y - 1,)),
        dma((G - 1,)), dma((G - 1,)),
        dma((Z - 1,)), dma((Z - 1,)),
        dma((slots,)), dma((slots,)),
    ]
    dx, gg, wg, bg = pl.pallas_call(
        functools.partial(kernel, (X, Z, C, Y)),
        out_shape=(
            jax.ShapeDtypeStruct((T, DL), BF16),
            jax.ShapeDtypeStruct((DL // 128, 128), F32),
            jax.ShapeDtypeStruct((columns, DL), F32),
            jax.ShapeDtypeStruct((O, H), F32),
        ),
        in_specs=[hbm] * 8,
        out_specs=(vmem,) * 4,
        scratch_shapes=scratch,
        compiler_params=pltpu.CompilerParams(
            collective_id=0, has_side_effects=True, vmem_limit_bytes=48 << 20
        ),
    )(
        *(
            pltpu.with_memory_space_constraint(a, pltpu.HBM)
            for a in (
                resid,
                head_in,
                norm_gain.reshape(1, DL),
                head_bias.reshape(1, N),
                head_out,
                targets.T,
                label_mask.T,
                obj_weight.reshape(1, O),
            )
        )
    )
    dx, gg, wg, bg = pl.pallas_call(
        settle,
        out_shape=tuple(jax.ShapeDtypeStruct(a.shape, a.dtype) for a in (dx, gg, wg, bg)),
        in_specs=[vmem] * 4,
        out_specs=(vmem,) * 4,
        compiler_params=pltpu.CompilerParams(vmem_limit_bytes=4 << 20),
    )(dx, gg, wg, bg)
    return dx, gg.reshape(DL), wg.T, bg.reshape(N)


def solution(mesh):
    finer = Mesh(mesh.devices.reshape(4, 8, 2, mesh.shape["tp"]), ("tok_0", "tok_1", "tok_2", "tp"))
    placed = (P(TOK, "tp"), P("tp"), P("tp", None), P(), P(), P(TOK, None), P(TOK, None), P())
    return jax.shard_map(
        per_device,
        mesh=finer,
        in_specs=placed,
        out_specs=(P(TOK, "tp"), P("tp"), P("tp", TOK), P()),
        check_vma=False,
    )
```
